32 devices in a mesh: dom: 4 (over z), col: 4 (over y, core), rep: 2 (over x).
Axes of the slice: x: 2, y: 2, z: 4, core: 2. Of those that a mesh axis runs over, the one named last changes fastest.
Arguments:
- features: bfloat16 [2, 4096, 100], P('rep', 'dom'), may hold values from -6 to 6
- w_in: bfloat16 [100, 256], P(None, 'col'), may hold values from -0.625 to 0.625
- w_hidden: bfloat16 [256, 256], P('col'), may hold values from -0.375 to 0.375
- blocks: bfloat16 [2, 4, 8, 512, 512], P('rep', 'dom'), may hold values from -0.125 to 0.125
- block_list: int32 [2, 4, 8, 3], P('rep', 'dom'), may hold values from 0 to 3, as said below
- block_count: int32 [2, 4], P('rep', 'dom'), may hold values from 1 to 8, as said below
- cotangent: bfloat16 [2, 4096, 256], P('rep', 'dom', 'col'), may hold values from -6 to 6
Outputs:
- out_hidden: bfloat16 [2, 4096, 256], P('rep', 'dom', 'col')
- grad_hidden: float32 [256, 256], P('col', ('dom', 'rep'))
The draws below stay inside these ranges and needn't reach their ends.
Inputs may be any that keep to these rules, and one draw needn't show every extreme that they name: `block_list`: each slot holds a row cluster below 2, a partner partition below 4 and a partner cluster below 2; the same cluster pair may stand in several slots, and then their blocks add. `block_count`: in every batch some partition uses all 8 slots.
All inputs are finite; a program needn't handle non-finite values.
Results may differ from the reference program's by a relative error of at most 0.0065.
Values may be sent and summed in bfloat16 or wider, within the bound.
No kernel may reach another device: no remote copies, remote signals or barrier semaphores. Data moves between devices by JAX's collectives and lax.ppermute only.
A program may use at most 64 MiB of HBM per device.

```python
import jax
import jax.numpy as jnp
from jax import lax

FEATS = 100
HID = 256
CLUS = 512
SLOTS = 8
CL_DEV = 2
NODES = 4096
N_DOM = 4
N_REP = 2


def draw_block_list(key, part):
    first, second, third = jax.random.split(jax.random.fold_in(key, 11), 3)
    shape = (N_REP, N_DOM, SLOTS)
    row_cluster = jax.random.randint(first, shape, 0, CL_DEV)
    partner = jax.random.randint(second, shape, 0, N_DOM)
    partner_cluster = jax.random.randint(third, shape, 0, CL_DEV)
    return jnp.stack([row_cluster, partner, partner_cluster], axis=-1).astype(jnp.int32)


def draw_block_count(key, part):
    first, second = jax.random.split(jax.random.fold_in(key, 23))
    counts = jax.random.randint(first, (N_REP, N_DOM), 1, SLOTS + 1)
    busiest = jax.random.randint(second, (N_REP,), 0, N_DOM)
    hit = jnp.arange(N_DOM)[None, :] == busiest[:, None]
    return jnp.where(hit, SLOTS, counts).astype(jnp.int32)


def shard_levels(stream_key, shape, pieces, smallest, top_value):
    level, own = 1.0, jax.random.fold_in(stream_key, 6)
    for dim, shards_of in pieces:
        steps = jnp.exp(jax.random.uniform(jax.random.fold_in(own, dim), (shards_of,), jnp.float32, smallest / len(pieces), top_value / len(pieces)))
        level = level * jnp.repeat(steps, shape[dim] // shards_of).reshape([-1 if axis == dim else 1 for axis in range(len(shape))])
    return level


def normal_values(key, dims, deviation, reach, cuts=(), kind=jnp.bfloat16):
    values = jax.random.normal(key, dims, jnp.float32) * deviation
    if len(cuts) > 0:
        values = shard_levels(key, dims, cuts, -0.22, 0.18) * values
    return jnp.clip(values, min=-reach, max=reach).astype(kind)


def setup_inputs(seed: int = 0) -> dict:
    streams_of = jax.random.split(jax.random.key(seed), 8)
    features = normal_values(streams_of[0], (N_REP, NODES, FEATS), 1.0, 6.0, ((0, 2), (1, 4)))
    w_in = normal_values(streams_of[1], (FEATS, HID), FEATS ** -0.5, 0.625, ((1, 4),))
    w_hidden = normal_values(streams_of[2], (HID, HID), HID ** -0.5, 0.375, ((0, 4),))
    blocks = normal_values(streams_of[3], (N_REP, N_DOM, SLOTS, CLUS, CLUS), (4 * CLUS) ** -0.5, 0.125, ((0, 2), (1, 4)))
    block_list = draw_block_list(jax.random.fold_in(streams_of[7], 71), 0)
    block_count = draw_block_count(jax.random.fold_in(streams_of[7], 71), 0)
    cotangent = normal_values(streams_of[6], (N_REP, NODES, HID), 1.0, 6.0, ((0, 2), (1, 4), (2, 4)))
    return {"features": features, "w_in": w_in, "w_hidden": w_hidden, "blocks": blocks, "block_list": block_list, "block_count": block_count, "cotangent": cotangent}


def slot_tables(block_list, block_count):
    rows_dev = CL_DEV * CLUS
    lists = block_list.reshape(N_DOM * SLOTS, 3).astype(jnp.int32)
    owner = jnp.repeat(jnp.arange(N_DOM, dtype=jnp.int32), SLOTS)
    live = (jnp.arange(SLOTS, dtype=jnp.int32)[None, :] < block_count[:, None]).reshape(-1)
    target = (owner * rows_dev + lists[:, 0] * CLUS).astype(jnp.int32)
    source = (lists[:, 1] * rows_dev + lists[:, 2] * CLUS).astype(jnp.int32)
    return target, source, live


def propagate(flat_blocks, target, source, live, values, adjoint):
    width = values.shape[1]
    total = jnp.zeros((values.shape[0], width), jnp.float32)

    def one(acc, item):
        block, into, frm, used = item
        if adjoint:
            frm, into = into, frm
            part = lax.dynamic_slice_in_dim(values, frm, CLUS, 0)
            term = lax.dot_general(block, part, (((0,), (0,)), ((), ())), preferred_element_type=jnp.float32)
        else:
            part = lax.dynamic_slice_in_dim(values, frm, CLUS, 0)
            term = jnp.dot(block, part, preferred_element_type=jnp.float32)
        term = jnp.where(used, term, jnp.zeros_like(term))
        current = lax.dynamic_slice_in_dim(acc, into, CLUS, 0)
        return lax.dynamic_update_slice_in_dim(acc, current + term, into, 0), None

    total, _ = lax.scan(one, total, (flat_blocks, target, source, live))
    return total


def one_batch(item, w_in, w_hidden):
    feats, blocks, block_list, block_count, cotangent = item
    flat_blocks = blocks.reshape(N_DOM * SLOTS, CLUS, CLUS)
    target, source, live = slot_tables(block_list, block_count)
    z1 = jnp.dot(feats, w_in, preferred_element_type=jnp.float32).astype(jnp.bfloat16)
    p1 = propagate(flat_blocks, target, source, live, z1, False)
    h1 = jax.nn.gelu(p1, approximate=True).astype(jnp.bfloat16)
    z2 = jnp.dot(h1, w_hidden, preferred_element_type=jnp.float32).astype(jnp.bfloat16)
    p2 = propagate(flat_blocks, target, source, live, z2, False).astype(jnp.bfloat16)
    dz2 = propagate(flat_blocks, target, source, live, cotangent, True).astype(jnp.bfloat16)
    grad = lax.dot_general(h1, dz2, (((0,), (0,)), ((), ())), preferred_element_type=jnp.float32)
    return p2, grad


def reference(features, w_in, w_hidden, blocks, block_list, block_count, cotangent):
    outs, grads = lax.map(lambda item: one_batch(item, w_in, w_hidden), (features, blocks, block_list, block_count, cotangent))
    return outs, jnp.sum(grads, axis=0)
```

```python
import functools
import math

import jax
import jax.numpy as jnp
from jax import lax
from jax.experimental import pallas as pl
from jax.experimental.pallas import tpu as pltpu
from jax.sharding import PartitionSpec as P


BF = jnp.bfloat16
F32 = jnp.float32
VM = pl.BlockSpec(memory_space=pltpu.VMEM)
SM = pl.BlockSpec(memory_space=pltpu.SMEM)
HB = pl.BlockSpec(memory_space=pl.ANY)
LANES = 128


def dot(a, b):
    return jnp.dot(a, b, preferred_element_type=F32)


def call(kernel, name, ins, specs, outs, scratch=(), flops=0, limit=24 << 20):
    return pl.pallas_call(
        kernel,
        name=name,
        out_shape=outs,
        in_specs=specs,
        out_specs=jax.tree.map(lambda _: VM, outs),
        scratch_shapes=list(scratch),
        compiler_params=pltpu.CompilerParams(vmem_limit_bytes=limit),
        cost_estimate=pl.CostEstimate(flops=flops, bytes_accessed=1 << 20, transcendentals=0),
    )(*ins)


def load_blocks(blocks, held, sems, count, slots):
    def copy(k):
        return pltpu.make_async_copy(blocks.at[0, 0, k], held.at[k], sems.at[k])

    for k in range(slots):
        pl.when(k < count)(lambda k=k: copy(k).start())
    return copy


def pack_kernel(feats, w_in, w_hid, xp, *wps, n_col, per, lane, groups):
    c = lax.axis_index("col")
    nodes, n_feat = feats.shape[1:]
    span = nodes // groups
    width = w_in.shape[1]
    row = lax.broadcasted_iota(jnp.int32, (n_feat, LANES), 0)
    col = lax.broadcasted_iota(jnp.int32, (n_feat, LANES), 1)
    total = None
    for g in range(groups):
        inner = col - g * lane
        pick = (inner >= 0) & (inner < per) & (row == c * per + inner)
        part = dot(feats[0, g * span : (g + 1) * span, :], pick.astype(F32).astype(BF))
        total = part if total is None else total + part
    xp[...] = total.astype(BF)
    hid = w_hid.shape[1]
    r2 = lax.broadcasted_iota(jnp.int32, (hid, width), 0)
    c2 = lax.broadcasted_iota(jnp.int32, (hid, width), 1)
    for t in range(n_col):
        to = lax.rem(c + t, n_col)
        pick = (r2 == c2 + to * width).astype(F32).astype(BF)
        wps[t][...] = jnp.zeros(wps[t].shape, BF)
        wps[t][:n_feat, :width] = w_in[...]
        wps[t][: w_hid.shape[0], width:] = dot(w_hid[...], pick).astype(BF)


def spread_kernel(lst, cnt, cot, blocks, *refs, n_dom, slots, clus, width):
    outs = refs[:n_dom]
    held, acc, turned, sems = refs[n_dom:]
    count = cnt[0, 0]
    copy = load_blocks(blocks, held, sems, count, slots)
    p = lax.axis_index("dom")
    cl = turned.shape[0]
    acc[...] = jnp.zeros(acc.shape, F32)
    for i in range(cl):
        turned[i] = cot[0, i * clus : (i + 1) * clus, :].astype(F32).T.astype(BF)
    for k in range(slots):

        @pl.when(k < count)
        def _(k=k):
            i = lst[0, 0, k, 0]
            at = lax.rem(lst[0, 0, k, 1] - p + n_dom, n_dom) * cl + lst[0, 0, k, 2]
            copy(k).wait()
            acc[at] += dot(turned[i], held[k])

    for s in range(n_dom):
        for j in range(cl):
            outs[s][j * width : (j + 1) * width, :] = acc[s * cl + j].astype(outs[s].dtype)


def weight_kernel(*refs, n_col, n_feat, per, lane, groups):
    wps = refs[:n_col]
    wst, wh = refs[n_col:]
    c = lax.axis_index("col")
    width = wh.shape[1]
    full = jnp.concatenate([w[:n_feat, :width] for w in wps], axis=1)
    l = lax.broadcasted_iota(jnp.int32, (LANES, n_feat), 0)
    u = lax.broadcasted_iota(jnp.int32, (LANES, n_feat), 1)
    l2 = lax.broadcasted_iota(jnp.int32, (LANES, full.shape[1]), 0)
    inner = lax.rem(l, lane)
    for t in range(n_col):
        frm = lax.rem(c - t + n_col, n_col)
        pick = ((inner < per) & (u == frm * per + inner)).astype(F32).astype(BF)
        base = dot(pick, full)
        for g in range(groups):
            keep = (l2 >= g * lane) & (l2 < (g + 1) * lane)
            wst[g, t * LANES : (t + 1) * LANES, :] = jnp.where(keep, base, 0.0).astype(BF)
        wh[t * width : (t + 1) * width, :] = wps[t][:width, width:]


def fold(lst, cnt, copy, held, src, acc, n_dom, slots):
    p = lax.axis_index("dom")
    cl = acc.shape[0]
    count = cnt[0, 0]
    for k in range(slots):

        @pl.when(k < count)
        def _(k=k):
            i = lst[0, 0, k, 0]
            at = lax.rem(p - lst[0, 0, k, 1] + n_dom, n_dom) * cl + lst[0, 0, k, 2]
            copy(k).wait()
            acc[i] += dot(held[k], src[at])


def first_kernel(lst, cnt, blocks, *refs, n_dom, slots, clus, lane, groups):
    xs = refs[:n_dom]
    out, held, src, acc, sems = refs[n_dom:]
    copy = load_blocks(blocks, held, sems, cnt[0, 0], slots)
    cl = acc.shape[0]
    span = out.shape[0]
    each = groups // cl
    for s in range(n_dom):
        for g in range(groups):
            at = (g % each) * span
            src[s * cl + g // each, at : at + span, :] = xs[s][:, g * lane : (g + 1) * lane]
    acc[...] = jnp.zeros(acc.shape, F32)
    fold(lst, cnt, copy, held, src, acc, n_dom, slots)
    for g in range(groups):
        at = (g % each) * span
        out[:, g * lane : (g + 1) * lane] = acc[g // each, at : at + span, :].astype(BF)


def gelu(v):
    return 0.5 * v * (1.0 + jnp.tanh(math.sqrt(2.0 / math.pi) * (v + 0.044715 * v * v * v)))


def hidden_kernel(*refs, n_col, groups, clus):
    axs = refs[:n_col]
    wst, wh, h1, zp = refs[n_col:]
    span = axs[0].shape[0]
    width = wh.shape[1]
    each = clus // span
    left = jnp.concatenate([a[...] for a in axs], axis=1)
    for g in range(groups):
        h = gelu(dot(left, wst[g])).astype(BF)
        h1[g * span : (g + 1) * span, :] = h
        z = dot(h, wh[...]).astype(BF)
        at = (g % each) * span
        j = g // each
        zp[at : at + span, j * width : (j + 1) * width] = z


def grad_kernel(*refs, n_dom, n_col, n_rep, clus, width, wj, packs):
    ys = refs[:n_dom]
    h1 = refs[n_dom]
    outs = refs[n_dom + 1 : -1]
    store = refs[-1]
    d, c, r = lax.axis_index("dom"), lax.axis_index("col"), lax.axis_index("rep")
    total = ys[0][...]
    for y in ys[1:]:
        total = total + y[...].astype(F32)
    dz = total.astype(BF)
    cl = dz.shape[0] // width
    g = None
    for j in range(cl):
        part = dot(dz[j * width : (j + 1) * width, :], h1[j * clus : (j + 1) * clus, :])
        g = part if g is None else g + part
    rows = wj // packs
    for t in range(n_col):
        for b in range(n_rep):
            piece = g[b * wj : (b + 1) * wj, t * width : (t + 1) * width]
            for m in range(packs):
                store[t * n_rep + b, :, m * width : (m + 1) * width] = piece[m * rows : (m + 1) * rows, :]
    for a in range(n_col):
        t = lax.rem(c - d - a + 2 * n_col, n_col)
        for b in range(n_rep):
            outs[a * n_rep + b][...] = store[t * n_rep + lax.rem(r + b, n_rep)]


def second_kernel(lst, cnt, blocks, *refs, n_dom, slots, clus):
    zs = refs[:n_dom]
    out, held, src, acc, sems = refs[n_dom:]
    copy = load_blocks(blocks, held, sems, cnt[0, 0], slots)
    cl = acc.shape[0]
    width = acc.shape[2]
    for s in range(n_dom):
        for j in range(cl):
            src[s * cl + j] = zs[s][:, j * width : (j + 1) * width]
    acc[...] = jnp.zeros(acc.shape, F32)
    fold(lst, cnt, copy, held, src, acc, n_dom, slots)
    for i in range(cl):
        out[0, i * clus : (i + 1) * clus, :] = acc[i].astype(BF)


def sum_kernel(*refs, packs, width):
    pieces = refs[:-1]
    out = refs[-1]
    total = pieces[0][...]
    for piece in pieces[1:]:
        total = total + piece[...]
    flat = jnp.concatenate([total[:, m * width : (m + 1) * width] for m in range(packs)], axis=0)
    out[...] = flat.T


def shifted(x, axis, size, s):
    return lax.ppermute(x, axis, [(i, (i + s) % size) for i in range(size)])


def body(features, w_in, w_hidden, blocks, block_list, block_count, cotangent):
    n_dom, n_col, n_rep = lax.axis_size("dom"), lax.axis_size("col"), lax.axis_size("rep")
    nodes, n_feat = features.shape[1:]
    slots, clus = blocks.shape[2], blocks.shape[3]
    cl = nodes // clus
    width = w_in.shape[1]
    hid = width * n_col
    per = -(-n_feat // n_col)
    lane = 1 << (per - 1).bit_length()
    groups = LANES // lane
    span = nodes // groups
    wj = hid // (n_dom * n_rep)
    assert n_dom == n_col and clus % span == 0 and wj * n_rep == width
    packs = LANES // width if wj % (8 * (LANES // width)) == 0 else 1
    sds = jax.ShapeDtypeStruct
    wrows = -(-max(n_feat, width) // 16) * 16
    block_flops = 2 * slots * clus * clus

    packed = call(
        functools.partial(pack_kernel, n_col=n_col, per=per, lane=lane, groups=groups),
        "pack",
        (features, w_in, w_hidden),
        [VM] * 3,
        [sds((span, LANES), BF)] + [sds((wrows, 2 * width), BF)] * n_col,
        flops=2 * nodes * n_feat * LANES,
    )
    xs = [packed[0]] + [shifted(packed[0], "dom", n_dom, s) for s in range(1, n_dom)]
    wps = [packed[1]] + [shifted(packed[1 + t], "col", n_col, t) for t in range(1, n_col)]

    held = pltpu.VMEM((slots, clus, clus), BF)
    sems = pltpu.SemaphoreType.DMA((slots,))
    ys = call(
        functools.partial(spread_kernel, n_dom=n_dom, slots=slots, clus=clus, width=width),
        "spread",
        (block_list, block_count, cotangent, blocks),
        [SM, SM, VM, HB],
        [sds((cl * width, clus), F32)] + [sds((cl * width, clus), BF)] * (n_dom - 1),
        [held, pltpu.VMEM((n_dom * cl, width, clus), F32), pltpu.VMEM((cl, width, clus), BF), sems],
        flops=block_flops * 256,
    )
    ys = [ys[0]] + [shifted(ys[s], "dom", n_dom, s) for s in range(1, n_dom)]
    wst, wh = call(
        functools.partial(weight_kernel, n_col=n_col, n_feat=n_feat, per=per, lane=lane, groups=groups),
        "weights",
        wps,
        [VM] * n_col,
        [sds((groups, n_col * LANES, hid), BF), sds((hid, width), BF)],
        flops=2 * n_col * LANES * n_feat * hid,
    )
    axp = call(
        functools.partial(first_kernel, n_dom=n_dom, slots=slots, clus=clus, lane=lane, groups=groups),
        "first",
        (block_list, block_count, blocks, *xs),
        [SM, SM, HB] + [VM] * n_dom,
        sds((span, LANES), BF),
        [held, pltpu.VMEM((n_dom * cl, clus, lane), BF), pltpu.VMEM((cl, clus, lane), F32), sems],
        flops=block_flops * 256,
    )
    axs = [axp] + [shifted(axp, "col", n_col, t) for t in range(1, n_col)]
    h1, zp = call(
        functools.partial(hidden_kernel, n_col=n_col, groups=groups, clus=clus),
        "hidden",
        (*axs, wst, wh),
        [VM] * (n_col + 2),
        [sds((nodes, hid), BF), sds((clus, cl * width), BF)],
        flops=2 * nodes * n_col * LANES * hid * 4,
    )
    zs = [zp] + [shifted(zp, "dom", n_dom, s) for s in range(1, n_dom)]
    pieces = call(
        functools.partial(
            grad_kernel, n_dom=n_dom, n_col=n_col, n_rep=n_rep, clus=clus, width=width, wj=wj, packs=packs
        ),
        "grad",
        (*ys, h1),
        [VM] * (n_dom + 1),
        [sds((wj // packs, packs * width), F32)] * (n_col * n_rep),
        [pltpu.VMEM((n_col * n_rep, wj // packs, packs * width), F32)],
        flops=2 * nodes * hid * width * 4,
    )
    grads = []
    for a in range(n_col):
        for b in range(n_rep):
            pairs = []
            for d in range(n_dom):
                for c in range(n_col):
                    for r in range(n_rep):
                        to = (c * n_col + (d + a) % n_col) * n_rep + (r + b) % n_rep
                        pairs.append(((d * n_col + c) * n_rep + r, to))
            grads.append(lax.ppermute(pieces[a * n_rep + b], ("dom", "col", "rep"), pairs))
    out = call(
        functools.partial(second_kernel, n_dom=n_dom, slots=slots, clus=clus),
        "second",
        (block_list, block_count, blocks, *zs),
        [SM, SM, HB] + [VM] * n_dom,
        sds((1, nodes, width), BF),
        [held, pltpu.VMEM((n_dom * cl, clus, width), BF), pltpu.VMEM((cl, clus, width), F32), sems],
        flops=block_flops * 256,
    )
    grad = call(
        functools.partial(sum_kernel, packs=packs, width=width),
        "total",
        grads,
        [VM] * len(grads),
        sds((width, wj), F32),
        flops=1000,
    )
    return out, grad


def solution(mesh):
    placed = (
        P("rep", "dom", None),
        P(None, "col"),
        P("col", None),
        P("rep", "dom", None, None, None),
        P("rep", "dom", None, None),
        P("rep", "dom"),
        P("rep", "dom", "col"),
    )
    return jax.shard_map(
        body,
        mesh=mesh,
        in_specs=placed,
        out_specs=(P("rep", "dom", "col"), P("col", ("dom", "rep"))),
        check_vma=False,
    )
```

```python
import functools
import math

import jax
import jax.numpy as jnp
from jax import lax
from jax.experimental import pallas as pl
from jax.experimental.pallas import tpu as pltpu
from jax.sharding import PartitionSpec as P


BF = jnp.bfloat16
F32 = jnp.float32
VM = pl.BlockSpec(memory_space=pltpu.VMEM)
SM = pl.BlockSpec(memory_space=pltpu.SMEM)
HB = pl.BlockSpec(memory_space=pltpu.HBM)
LANES = 128
LIM = 24 << 20
SPREAD_LIM = 50 << 20
ROWS = 16


def dot(a, b):
    return jnp.dot(a, b, preferred_element_type=F32)


def call(kernel, ins, specs, outs, scratch=(), flops=0, limit=24 << 20):
    return pl.pallas_call(
        kernel,
        out_shape=outs,
        in_specs=specs,
        out_specs=jax.tree.map(lambda _: VM, outs),
        scratch_shapes=list(scratch),
        compiler_params=pltpu.CompilerParams(vmem_limit_bytes=limit),
        cost_estimate=pl.CostEstimate(flops=flops, bytes_accessed=1 << 20, transcendentals=0),
    )(*ins)


def tables(lst, cnt, lst_s, cnt_s, sems):
    return [pltpu.make_async_copy(lst, lst_s, sems.at[0]), pltpu.make_async_copy(cnt, cnt_s, sems.at[1])]


def ndot(a, b):
    return lax.dot_general(a, b, (((1,), (1,)), ((), ())), preferred_element_type=F32)


def onehot(mask):
    return mask.astype(F32).astype(BF)


def pack_kernel(feats_h, w_in_h, w_hid_h, xp, *refs, n_col, per, lane):
    wps = refs[:n_col]
    feats, w_in, w_hid, h_abs, sems = refs[n_col:]
    pairs = ((feats_h, feats), (w_in_h, w_in), (w_hid_h, w_hid))
    copies = [pltpu.make_async_copy(a, b, sems.at[n]) for n, (a, b) in enumerate(pairs)]
    for copy in copies:
        copy.start()
    c = lax.axis_index("col")
    n_feat = feats.shape[1]
    width = w_in.shape[0]
    row = lax.broadcasted_iota(jnp.int32, (lane, n_feat), 0)
    col = lax.broadcasted_iota(jnp.int32, (lane, n_feat), 1)
    mine = onehot((row < per) & (col == c * per + row))
    frow = lax.broadcasted_iota(jnp.int32, (n_feat, LANES), 0)
    fcol = lax.broadcasted_iota(jnp.int32, (n_feat, LANES), 1)
    inner = lax.rem(fcol, lane)
    every = onehot((inner < per) & (frow == (fcol // lane) * per + inner))
    for copy in copies:
        copy.wait()
    xp[...] = dot(mine, feats[0]).astype(BF)
    spread = dot(w_in[...], every).astype(BF)
    turned = w_hid[...].astype(F32).T.astype(BF)
    for t in range(n_col):
        h_abs[t] = turned[t * width : (t + 1) * width, :]
    for t in range(n_col):
        part = h_abs[lax.rem(c + t, n_col)]
        wps[t][...] = jnp.zeros(wps[t].shape, BF)
        for m in range(width // ROWS):
            rows = slice(m * ROWS, (m + 1) * ROWS)
            wps[t][:, 2 * m * LANES : (2 * m + 1) * LANES] = spread[rows, :]
            wps[t][:, (2 * m + 1) * LANES : (2 * m + 1) * LANES + width] = part[rows, :]


def spread_kernel(lst_h, cnt_h, cot_h, blocks, *refs, n_dom, slots, clus, width):
    outs = refs[:n_dom]
    lst, cnt, cot, held, acc, small, sems = refs[n_dom:]
    first = tables(lst_h, cnt_h, lst, cnt, small) + [pltpu.make_async_copy(cot_h, cot, small.at[2])]
    copies = [pltpu.make_async_copy(blocks.at[0, 0, k], held.at[k], sems.at[k]) for k in range(slots)]
    for copy in first + copies:
        copy.start()
    p = lax.axis_index("dom")
    cl = acc.shape[0] // n_dom
    acc[...] = jnp.zeros(acc.shape, F32)
    for copy in first:
        copy.wait()
    for k in range(slots):
        i = jnp.clip(lst[0, 0, 0, k], 0, cl - 1)
        at = lax.rem(lst[0, 1, 0, k] - p + n_dom, n_dom) * cl + lst[0, 2, 0, k]
        at = jnp.clip(at, 0, n_dom * cl - 1)
        left = cot[0, :, pl.ds(pl.multiple_of(i * clus, LANES), clus)]
        left = jnp.where(k < cnt[0, 0], left, jnp.zeros_like(left))
        copies[k].wait()
        acc[at] += dot(left, held[k])
    for s in range(n_dom):
        for j in range(cl):
            outs[s][:, j * clus : (j + 1) * clus] = acc[s * cl + j].astype(outs[s].dtype)


def fold(lst_h, cnt_h, held, lst, cnt, src, acc, small, fill, n_dom, slots):
    first = tables(lst_h, cnt_h, lst, cnt, small)
    for copy in first:
        copy.start()
    cl = acc.shape[0]
    p = lax.axis_index("dom")
    fill()
    acc[...] = jnp.zeros(acc.shape, F32)
    for copy in first:
        copy.wait()
    for k in range(slots):
        i = jnp.clip(lst[0, 0, 0, k], 0, cl - 1)
        at = lax.rem(p - lst[0, 1, 0, k] + n_dom, n_dom) * cl + lst[0, 2, 0, k]
        left = src[jnp.clip(at, 0, n_dom * cl - 1)]
        left = jnp.where(k < cnt[0, 0], left, jnp.zeros_like(left))
        acc[i] += ndot(left, held[0, 0, k])


def first_kernel(lst_h, cnt_h, held, *refs, n_dom, n_col, slots, clus, cl, lane):
    xs = refs[:n_dom]
    wps = refs[n_dom : n_dom + n_col]
    outs = refs[n_dom + n_col : n_dom + 2 * n_col]
    lst, cnt, src, acc, small = refs[n_dom + 2 * n_col :]

    def fill():
        for s in range(n_dom):
            for j in range(cl):
                src[s * cl + j] = xs[s][:, j * clus : (j + 1) * clus]
        for t in range(n_col):
            outs[t][lane:, :] = wps[t][...]

    fold(lst_h, cnt_h, held, lst, cnt, src, acc, small, fill, n_dom, slots)
    for i in range(cl):
        part = acc[i].astype(BF)
        for t in range(n_col):
            outs[t][:lane, i * clus : (i + 1) * clus] = part


def gelu(v):
    return 0.5 * v * (1.0 + jnp.tanh(math.sqrt(2.0 / math.pi) * (v + 0.044715 * v * v * v)))


def hidden_kernel(*refs, n_col, lane, width):
    pays = refs[:n_col]
    h1, zp, ax, w1, w2 = refs[n_col:]
    c = lax.axis_index("col")
    for t in range(n_col):
        frm = lax.rem(c - t + n_col, n_col)
        ax[frm] = pays[t][:lane, :]
        for m in range(width // ROWS):
            rows = slice(m * ROWS, (m + 1) * ROWS)
            w1[frm, rows, :] = pays[t][lane:, 2 * m * LANES : (2 * m + 1) * LANES]
            w2[frm, rows, :] = pays[t][lane:, (2 * m + 1) * LANES : (2 * m + 1) * LANES + width]
    left = w1[...].reshape(n_col * width, LANES)
    out = jnp.concatenate([w2[t] for t in range(n_col)], axis=1)
    nodes = h1.shape[1]
    right = ax[...].reshape(n_col * lane, nodes)
    step = nodes // 4
    for m in range(4):
        cols = slice(m * step, (m + 1) * step)
        h = gelu(dot(left, right[:, cols])).astype(BF)
        h1[:, cols] = h
        zp[:, cols] = dot(out, h).astype(BF)


def grad_kernel(*refs, n_dom, n_rep, wj):
    ys = refs[:n_dom]
    h1 = refs[n_dom]
    outs = refs[n_dom + 1 : -1]
    store = refs[-1]
    r = lax.axis_index("rep")
    total = ys[0][...]
    for y in ys[1:]:
        total = total + y[...].astype(F32)
    g = ndot(total.astype(BF), h1[...])
    for b in range(n_rep):
        store[b] = g[b * wj : (b + 1) * wj, :]
    for b in range(n_rep):
        outs[b][...] = store[lax.rem(r + b, n_rep)]


def pieces_kernel(*refs, n_col, n_rep, width, packs):
    parts = refs[:n_rep]
    outs = refs[n_rep:-1]
    store = refs[-1]
    d = lax.axis_index("dom")
    g = parts[0][...]
    for part in parts[1:]:
        g = g + part[...]
    rows = g.shape[0] // packs
    for t in range(n_col):
        for m in range(packs):
            store[t, :, m * width : (m + 1) * width] = g[m * rows : (m + 1) * rows, t * width : (t + 1) * width]
    for a in range(n_col):
        outs[a][...] = store[lax.rem(d + a, n_col)]


def second_kernel(lst_h, cnt_h, held, *refs, n_dom, slots, clus, cl):
    zs = refs[:n_dom]
    out, lst, cnt, src, acc, small = refs[n_dom:]

    def fill():
        for s in range(n_dom):
            for j in range(cl):
                src[s * cl + j] = zs[s][:, j * clus : (j + 1) * clus]

    fold(lst_h, cnt_h, held, lst, cnt, src, acc, small, fill, n_dom, slots)
    for i in range(cl):
        out[0, :, i * clus : (i + 1) * clus] = acc[i].astype(BF)


def sum_kernel(*refs, packs, width):
    pieces = refs[:-1]
    out = refs[-1]
    total = pieces[0][...]
    for piece in pieces[1:]:
        total = total + piece[...]
    rows = total.shape[0]
    for m in range(packs):
        out[m * rows : (m + 1) * rows, :] = total[:, m * width : (m + 1) * width]


def shifted(x, axis, size, s):
    return lax.ppermute(x, axis, [(i, (i + s) % size) for i in range(size)])


def body(features, w_in, w_hidden, blocks, block_list, block_count, cotangent):
    n_dom, n_col, n_rep = lax.axis_size("dom"), lax.axis_size("col"), lax.axis_size("rep")
    features = jnp.swapaxes(features, 1, 2)
    cotangent = jnp.swapaxes(cotangent, 1, 2)
    w_in = w_in.T
    block_list = jnp.transpose(block_list, (0, 3, 1, 2))
    n_feat, nodes = features.shape[1:]
    slots, clus = blocks.shape[2], blocks.shape[3]
    cl = nodes // clus
    width = w_in.shape[0]
    hid = width * n_col
    per = -(-n_feat // n_col)
    lane = LANES // n_col
    wj = hid // (n_dom * n_rep)
    assert n_dom == n_col and wj * n_rep == width and width % ROWS == 0
    assert per <= lane and lane % ROWS == 0 and width <= LANES and 2 * LANES * (width // ROWS) <= nodes
    packs = LANES // width if wj % (8 * (LANES // width)) == 0 else 1
    sds = jax.ShapeDtypeStruct
    block_flops = 2 * slots * clus * clus

    slot_scratch = [
        pltpu.SMEM(block_list.shape, jnp.int32),
        pltpu.SMEM(block_count.shape, jnp.int32),
    ]
    sems = pltpu.SemaphoreType.DMA((slots,))
    small = pltpu.SemaphoreType.DMA((3,))
    packed = call(
        functools.partial(pack_kernel, n_col=n_col, per=per, lane=lane),
        (features, w_in, w_hidden),
        [HB] * 3,
        [sds((lane, nodes), BF)] + [sds((ROWS, nodes), BF)] * n_col,
        [
            pltpu.VMEM(features.shape, BF),
            pltpu.VMEM(w_in.shape, BF),
            pltpu.VMEM(w_hidden.shape, BF),
            pltpu.VMEM((n_col, width, width), BF),
            small,
        ],
        flops=2 * nodes * n_feat * LANES,
    )
    xs = [packed[0]] + [shifted(packed[0], "dom", n_dom, s) for s in range(1, n_dom)]
    ys = call(
        functools.partial(spread_kernel, n_dom=n_dom, slots=slots, clus=clus, width=width),
        (block_list, block_count, cotangent, blocks),
        [HB] * 4,
        [sds((width, nodes), F32)] + [sds((width, nodes), BF)] * (n_dom - 1),
        slot_scratch + [
            pltpu.VMEM(cotangent.shape, BF),
            pltpu.VMEM((slots, clus, clus), BF),
            pltpu.VMEM((n_dom * cl, width, clus), F32),
            small,
            sems,
        ],
        flops=block_flops * 256,
        limit=SPREAD_LIM,
    )
    ys = [ys[0]] + [shifted(ys[s], "dom", n_dom, s) for s in range(1, n_dom)]

    def fold_scratch(wide):
        return slot_scratch + [
            pltpu.VMEM((n_dom * cl, wide, clus), BF),
            pltpu.VMEM((cl, wide, clus), F32),
            small,
        ]

    pays = call(
        functools.partial(first_kernel, n_dom=n_dom, n_col=n_col, slots=slots, clus=clus, cl=cl, lane=lane),
        (block_list, block_count, blocks, *xs, *packed[1:]),
        [HB] * 2 + [VM] * (1 + n_dom + n_col),
        [sds((lane + ROWS, nodes), BF)] * n_col,
        fold_scratch(lane),
        flops=block_flops * 256,
        limit=LIM,
    )
    pays = [pays[0]] + [shifted(pays[t], "col", n_col, t) for t in range(1, n_col)]
    h1, zp = call(
        functools.partial(hidden_kernel, n_col=n_col, lane=lane, width=width),
        pays,
        [VM] * n_col,
        [sds((hid, nodes), BF), sds((width, nodes), BF)],
        [
            pltpu.VMEM((n_col, lane, nodes), BF),
            pltpu.VMEM((n_col, width, LANES), BF),
            pltpu.VMEM((n_col, width, width), BF),
        ],
        flops=2 * nodes * n_col * LANES * hid * 4,
    )
    zs = [zp] + [shifted(zp, "dom", n_dom, s) for s in range(1, n_dom)]
    halves = call(
        functools.partial(grad_kernel, n_dom=n_dom, n_rep=n_rep, wj=wj),
        (*ys, h1),
        [VM] * (n_dom + 1),
        [sds((wj, hid), F32)] * n_rep,
        [pltpu.VMEM((n_rep, wj, hid), F32)],
        flops=2 * nodes * hid * width * 4,
    )
    halves = [halves[0]] + [shifted(halves[b], "rep", n_rep, b) for b in range(1, n_rep)]
    pieces = call(
        functools.partial(pieces_kernel, n_col=n_col, n_rep=n_rep, width=width, packs=packs),
        halves,
        [VM] * n_rep,
        [sds((wj // packs, packs * width), F32)] * n_col,
        [pltpu.VMEM((n_col, wj // packs, packs * width), F32)],
        flops=1000,
    )
    grads = []
    for a in range(n_col):
        pairs = []
        for d in range(n_dom):
            for c in range(n_col):
                pairs.append((d * n_col + c, c * n_col + (d + a) % n_col))
        grads.append(lax.ppermute(pieces[a], ("dom", "col"), pairs))
    out = call(
        functools.partial(second_kernel, n_dom=n_dom, slots=slots, clus=clus, cl=cl),
        (block_list, block_count, blocks, *zs),
        [HB] * 2 + [VM] * (1 + n_dom),
        sds((1, width, nodes), BF),
        fold_scratch(width),
        flops=block_flops * 256,
        limit=LIM,
    )
    grad = call(
        functools.partial(sum_kernel, packs=packs, width=width),
        grads,
        [VM] * n_col,
        sds((wj, width), F32),
        flops=1000,
    )
    return jnp.swapaxes(out, 1, 2), grad.T


def solution(mesh):
    placed = (
        P("rep", "dom", None),
        P(None, "col"),
        P("col", None),
        P("rep", "dom", None, None, None),
        P("rep", "dom", None, None),
        P("rep", "dom"),
        P("rep", "dom", "col"),
    )

    return jax.shard_map(
        body,
        mesh=mesh,
        in_specs=placed,
        out_specs=(P("rep", "dom", "col"), P("col", ("dom", "rep"))),
        check_vma=False,
    )
```

```python
import functools
import math

import jax
import jax.numpy as jnp
from jax import lax
from jax.experimental import pallas as pl
from jax.experimental.pallas import tpu as pltpu
from jax.sharding import PartitionSpec as P


BF = jnp.bfloat16
F32 = jnp.float32
VM = pl.BlockSpec(memory_space=pltpu.VMEM)
SM = pl.BlockSpec(memory_space=pltpu.SMEM)
HB = pl.BlockSpec(memory_space=pltpu.HBM)
LANES = 128
LIM = 24 << 20
PICK_LIM = 50 << 20
ROWS = 16


def dot(a, b):
    return jnp.dot(a, b, preferred_element_type=F32)


def call(kernel, ins, specs, outs, scratch=(), flops=0, limit=24 << 20, spaces=None):
    return pl.pallas_call(
        kernel,
        out_shape=outs,
        in_specs=specs,
        out_specs=spaces or jax.tree.map(lambda _: VM, outs),
        scratch_shapes=list(scratch),
        compiler_params=pltpu.CompilerParams(vmem_limit_bytes=limit),
        cost_estimate=pl.CostEstimate(flops=flops, bytes_accessed=1 << 20, transcendentals=0),
    )(*ins)


def ndot(a, b):
    return lax.dot_general(a, b, (((1,), (1,)), ((), ())), preferred_element_type=F32)


def onehot(mask):
    return mask.astype(F32).astype(BF)


def pick_kernel(feats, _, xp, *, per, lane):
    c = lax.axis_index("col")
    n_feat = feats.shape[1]
    row = lax.broadcasted_iota(jnp.int32, (lane, n_feat), 0)
    col = lax.broadcasted_iota(jnp.int32, (lane, n_feat), 1)
    mine = onehot((row < per) & (col == c * per + row))
    xp[...] = dot(mine, feats[0]).astype(BF)


def pack_kernel(w_in, w_hid, *refs, n_col, per, lane):
    wps = refs[:n_col]
    h_abs = refs[n_col]
    c = lax.axis_index("col")
    width, n_feat = w_in.shape
    frow = lax.broadcasted_iota(jnp.int32, (n_feat, LANES), 0)
    fcol = lax.broadcasted_iota(jnp.int32, (n_feat, LANES), 1)
    inner = lax.rem(fcol, lane)
    every = onehot((inner < per) & (frow == (fcol // lane) * per + inner))
    spread = dot(w_in[...], every).astype(BF)
    turned = w_hid[...].astype(F32).T.astype(BF)
    for t in range(n_col):
        h_abs[t] = turned[t * width : (t + 1) * width, :]
    for t in range(n_col):
        part = h_abs[c ^ t]
        wps[t][...] = jnp.zeros(wps[t].shape, BF)
        for m in range(width // ROWS):
            rows = slice(m * ROWS, (m + 1) * ROWS)
            wps[t][:, 2 * m * LANES : (2 * m + 1) * LANES] = spread[rows, :]
            wps[t][:, (2 * m + 1) * LANES : (2 * m + 1) * LANES + width] = part[rows, :]


def spread_kernel(lst_h, cnt, cot, held, tab, *refs, n_dom, slots, clus):
    outs = refs[:n_dom]
    lst, acc, sem = refs[n_dom:]
    copy = pltpu.make_async_copy(lst_h, lst, sem)
    copy.start()
    p = lax.axis_index("dom")
    cl = acc.shape[0] // n_dom
    acc[...] = jnp.zeros(acc.shape, F32)
    copy.wait()
    for m in range(3):
        for k in range(slots):
            tab[0, m * slots + k] = lst[0, m, 0, k]
    tab[0, 3 * slots] = cnt[0, 0]
    for k in range(slots):
        i = jnp.clip(tab[0, k], 0, cl - 1)
        at = (tab[0, slots + k] ^ p) * cl + tab[0, 2 * slots + k]
        at = jnp.clip(at, 0, n_dom * cl - 1)
        left = cot[0, :, pl.ds(pl.multiple_of(i * clus, LANES), clus)]
        left = jnp.where(k < tab[0, 3 * slots], left, jnp.zeros_like(left))
        acc[at] += dot(left, held[0, 0, k])
    for s in range(n_dom):
        for j in range(cl):
            outs[s][:, j * clus : (j + 1) * clus] = acc[s * cl + j].astype(outs[s].dtype)


def fold(tab, held, src, acc, n_dom, slots):
    cl = acc.shape[0]
    p = lax.axis_index("dom")
    acc[...] = jnp.zeros(acc.shape, F32)
    for k in range(slots):
        i = jnp.clip(tab[0, k], 0, cl - 1)
        at = (tab[0, slots + k] ^ p) * cl + tab[0, 2 * slots + k]
        left = src[jnp.clip(at, 0, n_dom * cl - 1)]
        left = jnp.where(k < tab[0, 3 * slots], left, jnp.zeros_like(left))
        acc[i] += ndot(left, held[0, 0, k])


def first_kernel(tab, held, *refs, n_dom, n_col, slots, clus, cl, lane):
    xs = refs[:n_dom]
    wps = refs[n_dom : n_dom + n_col]
    outs = refs[n_dom + n_col : n_dom + 2 * n_col]
    src, acc = refs[n_dom + 2 * n_col :]

    for s in range(n_dom):
        for j in range(cl):
            src[s * cl + j] = xs[s][:, j * clus : (j + 1) * clus]
    for t in range(n_col):
        outs[t][lane:, :] = wps[t][...]
    fold(tab, held, src, acc, n_dom, slots)
    for i in range(cl):
        part = acc[i].astype(BF)
        for t in range(n_col):
            outs[t][:lane, i * clus : (i + 1) * clus] = part


def gelu(v):
    return 0.5 * v * (1.0 + jnp.tanh(math.sqrt(2.0 / math.pi) * (v + 0.044715 * v * v * v)))


def hidden_kernel(*refs, n_col, lane, width):
    pays = refs[:n_col]
    h1, zp, ax, w1, w2 = refs[n_col:]
    c = lax.axis_index("col")
    for t in range(n_col):
        frm = c ^ t
        ax[frm] = pays[t][:lane, :]
        for m in range(width // ROWS):
            rows = slice(m * ROWS, (m + 1) * ROWS)
            w1[frm, rows, :] = pays[t][lane:, 2 * m * LANES : (2 * m + 1) * LANES]
            w2[frm, rows, :] = pays[t][lane:, (2 * m + 1) * LANES : (2 * m + 1) * LANES + width]
    left = w1[...].reshape(n_col * width, LANES)
    out = jnp.concatenate([w2[t] for t in range(n_col)], axis=1)
    nodes = h1.shape[1]
    right = ax[...].reshape(n_col * lane, nodes)
    step = nodes // 4
    for m in range(4):
        cols = slice(m * step, (m + 1) * step)
        h = gelu(dot(left, right[:, cols])).astype(BF)
        h1[:, cols] = h
        zp[:, cols] = dot(out, h).astype(BF)


def grad_kernel(*refs, n_dom, n_rep, wj):
    ys = refs[:n_dom]
    h1 = refs[n_dom]
    outs = refs[n_dom + 1 : -1]
    store = refs[-1]
    r = lax.axis_index("rep")
    total = ys[0][...]
    for y in ys[1:]:
        total = total + y[...].astype(F32)
    g = ndot(total.astype(BF), h1[...])
    for b in range(n_rep):
        store[b] = g[b * wj : (b + 1) * wj, :]
    for b in range(n_rep):
        outs[b][...] = store[r ^ b]


def pieces_kernel(*refs, n_col, n_rep, width, packs):
    parts = refs[:n_rep]
    outs = refs[n_rep:-1]
    store = refs[-1]
    d = lax.axis_index("dom")
    g = parts[0][...]
    for part in parts[1:]:
        g = g + part[...]
    rows = g.shape[0] // packs
    for t in range(n_col):
        for m in range(packs):
            store[t, :, m * width : (m + 1) * width] = g[m * rows : (m + 1) * rows, t * width : (t + 1) * width]
    for a in range(n_col):
        outs[a][...] = store[d ^ a]


def second_kernel(tab, held, *refs, n_dom, slots, clus, cl):
    zs = refs[:n_dom]
    out, src, acc = refs[n_dom:]
    for s in range(n_dom):
        for j in range(cl):
            src[s * cl + j] = zs[s][:, j * clus : (j + 1) * clus]
    fold(tab, held, src, acc, n_dom, slots)
    for i in range(cl):
        out[0, :, i * clus : (i + 1) * clus] = acc[i].astype(BF)


def sum_kernel(*refs, packs, width):
    pieces = refs[:-1]
    out = refs[-1]
    total = pieces[0][...]
    for piece in pieces[1:]:
        total = total + piece[...]
    rows = total.shape[0]
    for m in range(packs):
        out[m * rows : (m + 1) * rows, :] = total[:, m * width : (m + 1) * width]


def shifted(x, axis, size, s):
    return lax.ppermute(x, axis, [(i, i ^ s) for i in range(size)])


def partners(x, axis, size):
    parts = x if isinstance(x, (list, tuple)) else [x] * size
    return [parts[0]] + [shifted(parts[s], axis, size, s) for s in range(1, size)]


def body(features, w_in, w_hidden, blocks, block_list, block_count, cotangent):
    n_dom, n_col, n_rep = lax.axis_size("dom"), lax.axis_size("col"), lax.axis_size("rep")
    features = jnp.swapaxes(features, 1, 2)
    cotangent = jnp.swapaxes(cotangent, 1, 2)
    w_in = w_in.T
    block_list = jnp.transpose(block_list, (0, 3, 1, 2))
    n_feat, nodes = features.shape[1:]
    slots, clus = blocks.shape[2], blocks.shape[3]
    cl = nodes // clus
    width = w_in.shape[0]
    hid = width * n_col
    per = -(-n_feat // n_col)
    lane = LANES // n_col
    wj = hid // (n_dom * n_rep)
    assert n_dom == n_col and n_dom & (n_dom - 1) == 0 and n_rep & (n_rep - 1) == 0
    assert wj * n_rep == width and width % ROWS == 0
    assert per <= lane and lane % ROWS == 0 and width <= LANES and 2 * LANES * (width // ROWS) <= nodes
    packs = LANES // width if wj % (8 * (LANES // width)) == 0 else 1
    sds = jax.ShapeDtypeStruct
    block_flops = 2 * slots * clus * clus

    xp = call(
        functools.partial(pick_kernel, per=per, lane=lane),
        (features, blocks),
        [VM, HB],
        sds((lane, nodes), BF),
        flops=2 * nodes * n_feat * LANES,
        limit=PICK_LIM,
    )
    xs = partners(xp, "dom", n_dom)
    tab, *ys = call(
        functools.partial(spread_kernel, n_dom=n_dom, slots=slots, clus=clus),
        (block_list, block_count, cotangent, blocks),
        [HB, VM, VM, VM],
        [sds((1, LANES), jnp.int32), sds((width, nodes), F32)] + [sds((width, nodes), BF)] * (n_dom - 1),
        [
            pltpu.SMEM(block_list.shape, jnp.int32),
            pltpu.VMEM((n_dom * cl, width, clus), F32),
            pltpu.SemaphoreType.DMA,
        ],
        flops=block_flops * 256,
        limit=LIM,
        spaces=[SM] + [VM] * n_dom,
    )
    wps = call(
        functools.partial(pack_kernel, n_col=n_col, per=per, lane=lane),
        (w_in, w_hidden),
        [VM, VM],
        [sds((ROWS, nodes), BF)] * n_col,
        [pltpu.VMEM((n_col, width, width), BF)],
        flops=1000,
    )

    def fold_scratch(wide):
        return [pltpu.VMEM((n_dom * cl, wide, clus), BF), pltpu.VMEM((cl, wide, clus), F32)]

    pays = call(
        functools.partial(first_kernel, n_dom=n_dom, n_col=n_col, slots=slots, clus=clus, cl=cl, lane=lane),
        (tab, blocks, *xs, *wps),
        [SM] + [VM] * (1 + n_dom + n_col),
        [sds((lane + ROWS, nodes), BF)] * n_col,
        fold_scratch(lane),
        flops=block_flops * 256,
        limit=LIM,
    )
    pays = partners(pays, "col", n_col)
    ys = partners(ys, "dom", n_dom)
    h1, zp = call(
        functools.partial(hidden_kernel, n_col=n_col, lane=lane, width=width),
        pays,
        [VM] * n_col,
        [sds((hid, nodes), BF), sds((width, nodes), BF)],
        [
            pltpu.VMEM((n_col, lane, nodes), BF),
            pltpu.VMEM((n_col, width, LANES), BF),
            pltpu.VMEM((n_col, width, width), BF),
        ],
        flops=2 * nodes * n_col * LANES * hid * 4,
    )
    zs = partners(zp, "dom", n_dom)
    halves = call(
        functools.partial(grad_kernel, n_dom=n_dom, n_rep=n_rep, wj=wj),
        (*ys, h1),
        [VM] * (n_dom + 1),
        [sds((wj, hid), F32)] * n_rep,
        [pltpu.VMEM((n_rep, wj, hid), F32)],
        flops=2 * nodes * hid * width * 4,
    )
    halves = partners(halves, "rep", n_rep)
    pieces = call(
        functools.partial(pieces_kernel, n_col=n_col, n_rep=n_rep, width=width, packs=packs),
        halves,
        [VM] * n_rep,
        [sds((wj // packs, packs * width), F32)] * n_col,
        [pltpu.VMEM((n_col, wj // packs, packs * width), F32)],
        flops=1000,
    )
    grads = []
    for a in range(n_col):
        pairs = []
        for d in range(n_dom):
            for c in range(n_col):
                pairs.append((d * n_col + c, c * n_col + (d ^ a)))
        grads.append(lax.ppermute(pieces[a], ("dom", "col"), pairs))
    out = call(
        functools.partial(second_kernel, n_dom=n_dom, slots=slots, clus=clus, cl=cl),
        (tab, blocks, *zs),
        [SM] + [VM] * (1 + n_dom),
        sds((1, width, nodes), BF),
        fold_scratch(width),
        flops=block_flops * 256,
        limit=LIM,
    )
    grad = call(
        functools.partial(sum_kernel, packs=packs, width=width),
        grads,
        [VM] * n_col,
        sds((wj, width), F32),
        flops=1000,
    )
    return jnp.swapaxes(out, 1, 2), grad.T


def solution(mesh):
    placed = (
        P("rep", "dom", None),
        P(None, "col"),
        P("col", None),
        P("rep", "dom", None, None, None),
        P("rep", "dom", None, None),
        P("rep", "dom"),
        P("rep", "dom", "col"),
    )

    return jax.shard_map(
        body,
        mesh=mesh,
        in_specs=placed,
        out_specs=(P("rep", "dom", "col"), P("col", ("dom", "rep"))),
        check_vma=False,
    )
```
